32 devices in a mesh: row: 4 (over y, x), col: 4 (over z), feat: 2 (over core).
Axes of the slice: x: 2, y: 2, z: 4, core: 2. Of those that a mesh axis runs over, the one named last changes fastest.
Arguments:
- points: bfloat16 [4, 4, 512, 1024], P(None, 'row', None, ('col', 'feat')), may hold values from -2 to 2
- point_noise: float32 [4, 4, 512], P(None, 'row'), may hold values from 0.1 to 1
Outputs:
- schur_tiles: float32 [4, 4, 512, 4, 4, 512], P(None, 'row', None, None, 'col', 'feat')
- trace_mean: float32 [], replicated
- log_diagonal: float32 [], replicated
The draws below stay inside these ranges and needn't reach their ends.
All inputs are finite; a program needn't handle non-finite values.
Results may differ from the reference program's by a relative error of at most 0.003.
Values may be sent and summed in bfloat16 or wider, within the bound.
No kernel may reach another device: no remote copies, remote signals or barrier semaphores. Data moves between devices by JAX's collectives and lax.ppermute only.
A program may use at most 128 MiB of HBM per device.

```python
import math
import jax
import jax.numpy as jnp
from jax import lax

TILE = 512
FEATURES = 1024
TILES_DEV = 4
N_ROW = 4
N_COL = 4


def draw_points(key, part):
    key_values = jax.random.fold_in(key, 11)
    key_rough = jax.random.fold_in(key, 23)
    tile_count = TILES_DEV * N_ROW
    tile_index = (jnp.arange(TILES_DEV)[:, None] * N_ROW + jnp.arange(N_ROW)[None, :]).astype(jnp.float32)
    scale_level = 0.6 * jnp.power(3.0, tile_index / max(tile_count - 1, 1))
    roughness = jax.random.uniform(key_rough, (TILES_DEV, N_ROW, TILE, 1), jnp.float32, 0.7, 1.4)
    entries = jnp.clip(jax.random.normal(key_values, (TILES_DEV, N_ROW, TILE, FEATURES), jnp.float32), -4.0, 4.0)
    values = entries * scale_level[:, :, None, None] * roughness / math.sqrt(32.0)
    return values.astype(jnp.bfloat16)


def block_levels(key, shape, cuts, smallest, top_value):
    def one(position, shards_of):
        heights = jax.random.uniform(jax.random.fold_in(jax.random.fold_in(key, 6), position), (shards_of,), jnp.float32, smallest / len(cuts), top_value / len(cuts))
        return jnp.repeat(jnp.exp(heights), shape[position] // shards_of).reshape((-1,) + (1,) * (len(shape) - position - 1))

    gain = one(*cuts[0])
    for cut in cuts[1:]:
        gain = gain * one(*cut)
    return gain


def setup_inputs(seed: int = 0) -> dict:
    seeds = jax.random.split(jax.random.key(seed), 3)
    return {
        "points": draw_points(jax.random.fold_in(seeds[2], 71), 0),
        "point_noise": jnp.clip(jnp.exp(math.log(1.0) - 2.3025851 * jax.random.uniform(seeds[1], (TILES_DEV, N_ROW, TILE), jnp.float32) ** block_levels(seeds[1], (TILES_DEV, N_ROW, TILE), ((1, 4),), -0.2, 0.2)), 0.1, 1.0),
    }


def reference(points, point_noise):
    tile_count = TILES_DEV * N_ROW
    point_count = tile_count * TILE
    all_points = points.reshape(point_count, FEATURES)
    gram_full = jnp.dot(all_points.astype(jnp.float32), all_points.T.astype(jnp.float32), preferred_element_type=jnp.float32)
    gram_full = gram_full + jnp.diag(point_noise.reshape(point_count).astype(jnp.float32))
    factor = jnp.linalg.cholesky(gram_full[:TILE, :TILE])
    inverse = jax.scipy.linalg.solve_triangular(factor, jnp.eye(TILE, dtype=jnp.float32), lower=True)
    panel_rows = jnp.dot(gram_full[:, :TILE], inverse.T, precision=lax.Precision.HIGHEST)
    schur_part = gram_full - jnp.dot(panel_rows, panel_rows.T, precision=lax.Precision.HIGHEST)
    schur_part = schur_part.at[:, :TILE].set(panel_rows)
    tile_index = (jnp.arange(point_count, dtype=jnp.int32) // TILE).astype(jnp.int32)
    lower_mask = tile_index[:, None] >= tile_index[None, :]
    schur_part = jnp.where(lower_mask, schur_part, jnp.float32(0.0))
    diagonal = jnp.diagonal(schur_part)[TILE:]
    trace_mean = jnp.sum(diagonal) / jnp.float32(point_count - TILE)
    log_diagonal = 2.0 * jnp.sum(jnp.log(jnp.diagonal(factor)))
    schur_tiles = schur_part.reshape(TILES_DEV, N_ROW, TILE, TILES_DEV, N_COL, TILE)
    return (schur_tiles, trace_mean, log_diagonal)
```

```python
import functools

import jax
import jax.numpy as jnp
from jax import lax
from jax.experimental import pallas as pl
from jax.experimental.pallas import tpu as pltpu
from jax.sharding import PartitionSpec as P


HIGHEST = lax.Precision.HIGHEST
NN = (((1,), (0,)), ((), ()))
NT = (((1,), (1,)), ((), ()))
TN = (((0,), (0,)), ((), ()))
GROUP = 8
BLOCK = 128
LANES = 128
CHUNK = 256
VMEM = pl.BlockSpec(memory_space=pltpu.VMEM)
ANY = pl.BlockSpec(memory_space=pl.ANY)


def split(x):
    high = x.astype(jnp.bfloat16)
    return high, (x - high.astype(jnp.float32)).astype(jnp.bfloat16)


def dot(a, b, dims, precision=None):
    return lax.dot_general(a, b, dims, precision=precision, preferred_element_type=jnp.float32)


class Layout:
    def __init__(self, width):
        self.cols, self.feats = lax.axis_size("col"), lax.axis_size("feat")
        self.apart = width % LANES == 0
        self.width = width if self.apart else width * self.feats
        self.inner = self.feats if self.apart else 1

    def offset(self, k, j):
        place = lax.rem(lax.axis_index("col") + (self.cols - k), self.cols) * self.inner
        if self.apart:
            place = place + lax.rem(lax.axis_index("feat") + j, self.feats)
        return pl.multiple_of(place * self.width, LANES)

    def units(self, parts):
        if self.apart:
            return parts
        turned = jnp.roll(jnp.stack(parts), lax.axis_index("feat"), axis=0)
        return [jnp.concatenate(list(turned), axis=-1)]


def factor_block(a_ref, w_ref):
    shape = (GROUP, BLOCK)
    sub = lax.broadcasted_iota(jnp.int32, shape, 0)

    def rows(x, k):
        return jnp.broadcast_to(x[k : k + 1, :], shape)

    def lanes(x, k):
        return jnp.broadcast_to(x[:, k : k + 1], shape)

    for first in range(0, BLOCK, GROUP):
        group = pl.ds(first, GROUP)
        a, w = a_ref[group, :], w_ref[group, :]
        cols = [lanes(a, first + j) for j in range(GROUP)]
        e = {(k, j): rows(cols[j], k) for j in range(GROUP) for k in range(j, GROUP)}
        inv, low = [], {}
        for j in range(GROUP):
            inv.append(lax.rsqrt(e[j, j]))
            for k in range(j + 1, GROUP):
                low[k, j] = e[k, j] * inv[j]
            for m in range(j + 1, GROUP):
                for k in range(m, GROUP):
                    e[k, m] = e[k, m] - low[k, j] * low[m, j]
        y, yw = [], []
        for k in range(GROUP):
            ra, rw = rows(a, k), rows(w, k)
            for j in range(k):
                ra = ra - low[k, j] * y[j]
                rw = rw - low[k, j] * yw[j]
            y.append(ra * inv[k])
            yw.append(rw * inv[k])
        na, nw = y[0], yw[0]
        for k in range(1, GROUP):
            na = jnp.where(sub == k, y[k], na)
            nw = jnp.where(sub == k, yw[k], nw)
        a_ref[group, :] = na
        w_ref[group, :] = nw
        for after in range(first + GROUP, BLOCK, GROUP):
            under = pl.ds(after, GROUP)
            a, w = a_ref[under, :], w_ref[under, :]
            c = []
            for j in range(GROUP):
                x = lanes(a, first + j)
                for m in range(j):
                    x = x - c[m] * low[j, m]
                c.append(x * inv[j])
            for j in range(GROUP):
                a = a - c[j] * y[j]
                w = w - c[j] * yw[j]
            a_ref[under, :] = a
            w_ref[under, :] = w


def factor_kernel(layout, *refs):
    *lead, noise_ref, qh_ref, ql_ref, l_ref, log_ref, p, a, w, da, dw, sems = refs
    size = a.shape[0]
    copies = []
    for j in range(layout.inner):
        for k in range(layout.cols):
            n = j * layout.cols + k
            there = p.at[:, pl.ds(layout.offset(k, j), layout.width)]
            copies.append(pltpu.make_async_copy(lead[j].at[k], there, sems.at[n]))
    for copy in copies:
        copy.start()
    for copy in copies:
        copy.wait()
    down = lax.broadcasted_iota(jnp.int32, (size, size), 0)
    across = lax.broadcasted_iota(jnp.int32, (size, size), 1)
    eye = down == across
    points = p[...]
    a[...] = dot(points, points, NT) + jnp.where(eye, noise_ref[...], 0.0)
    w[...] = jnp.where(eye, 1.0, 0.0)
    blocks = size // BLOCK

    def step(n, carry):
        at = pl.ds(pl.multiple_of(n * BLOCK, BLOCK), BLOCK)
        da[...] = a[at, at]
        dw[...] = w[at, at]
        factor_block(da, dw)
        a[at, at] = da[...]
        for m in range(blocks):
            lo, hi = m * BLOCK, (m + 1) * BLOCK

            @pl.when(n == m)
            def _():
                inverse = dw[...]
                if m:
                    w[lo:hi, :lo] = dot(inverse, w[lo:hi, :lo], NN, HIGHEST)
                w[lo:hi, lo:hi] = inverse
                if hi < size:
                    y = dot(inverse, a[lo:hi, hi:], NN, HIGHEST)
                    a[lo:hi, hi:] = y
                    a[hi:, hi:] = a[hi:, hi:] - dot(y, y, TN, HIGHEST)
                    w[hi:, :hi] = w[hi:, :hi] - dot(y, w[lo:hi, :hi], TN, HIGHEST)

        return carry

    lax.fori_loop(0, blocks, step, 0)
    upper = a[...]
    logs = jnp.where(eye, jnp.log(jnp.where(eye, upper, 1.0)), 0.0)
    log_ref[...] = jnp.broadcast_to(2.0 * jnp.sum(logs), log_ref.shape)
    l_ref[...] = jnp.where(down <= across, upper, 0.0).T
    inverse = jnp.where(down >= across, w[...], 0.0)
    first = inverse.astype(jnp.bfloat16)
    second, third = split(inverse - first.astype(jnp.float32))
    q = dot(first, points, NN) + dot(second, points, NN) + dot(third, points, NN)
    qh_ref[...], ql_ref[...] = split(q)


def factor(layout, lead, noise, features):
    size = noise.shape[-1]
    f32, bf16 = jnp.float32, jnp.bfloat16
    return pl.pallas_call(
        functools.partial(factor_kernel, layout),
        out_shape=(
            jax.ShapeDtypeStruct((size, features), bf16),
            jax.ShapeDtypeStruct((size, features), bf16),
            jax.ShapeDtypeStruct((size, size), f32),
            jax.ShapeDtypeStruct((8, LANES), f32),
        ),
        in_specs=[ANY] * len(lead) + [VMEM],
        out_specs=(VMEM,) * 4,
        scratch_shapes=[
            pltpu.VMEM((size, features), bf16),
            pltpu.VMEM((size, size), f32),
            pltpu.VMEM((size, size), f32),
            pltpu.VMEM((BLOCK, BLOCK), f32),
            pltpu.VMEM((BLOCK, BLOCK), f32),
            pltpu.SemaphoreType.DMA((layout.cols * layout.inner,)),
        ],
        compiler_params=pltpu.CompilerParams(vmem_limit_bytes=24 << 20),
        cost_estimate=pl.CostEstimate(
            flops=30 * 10**9, bytes_accessed=4 * 10**6, transcendentals=0
        ),
        name="factor",
    )(*lead, noise)


def panel_kernel(layout, tiles, features, *refs):
    count = layout.cols * layout.inner
    lead, rest = refs[: layout.inner], refs[layout.inner : layout.inner + count]
    qh_ref, ql_ref, l_ref, noise_ref, x_ref, trace_ref, sems = refs[layout.inner + count :]
    size = l_ref.shape[0]
    row = lax.axis_index("row")
    copies = []
    for j in range(layout.inner):
        for k in range(layout.cols):
            n = j * layout.cols + k
            lanes = pl.ds(layout.offset(k, j), layout.width)
            copies.append(
                pltpu.make_async_copy(lead[j].at[k], x_ref.at[0, :, lanes], sems.at[0, n])
            )
            if tiles > 1:
                copies.append(
                    pltpu.make_async_copy(
                        rest[n], x_ref.at[pl.ds(1, tiles - 1), :, lanes], sems.at[1, n]
                    )
                )
    for copy in copies:
        copy.start()
    for copy in copies:
        copy.wait()
    trace_ref[...] = jnp.zeros_like(trace_ref)

    def add(points, panel, noise):
        p = points.astype(jnp.float32)
        total = jnp.sum(p * p, axis=0, keepdims=True)
        taken = jnp.sum(panel * panel, axis=0, keepdims=True)
        fold = lambda x: functools.reduce(
            jnp.add, [x[:, n : n + LANES] for n in range(0, x.shape[1], LANES)]
        )
        trace_ref[0:1, :] = trace_ref[0:1, :] + ((fold(total) + fold(noise)) - fold(taken))

    for t in range(tiles):
        points = x_ref[t, :, :features]
        panel = dot(points, qh_ref[...], NT) + dot(points, ql_ref[...], NT)
        if t == 0:
            panel = jnp.where(row == 0, l_ref[...], panel)
        high, low = split(panel)
        x_ref[t, :, features : features + size] = high
        x_ref[t, :, features + size :] = low
        if t == 0:

            @pl.when(row > 0)
            def _():
                add(points, panel, noise_ref[t : t + 1, :])

        else:
            add(points, panel, noise_ref[t : t + 1, :])


def row_panel(layout, lead, rest, factors, noise):
    qh, ql, low = factors
    tiles, size = noise.shape
    features = qh.shape[1]
    count = layout.cols * layout.inner
    return pl.pallas_call(
        functools.partial(panel_kernel, layout, tiles, features),
        out_shape=(
            jax.ShapeDtypeStruct((tiles, size, features + 2 * size), jnp.bfloat16),
            jax.ShapeDtypeStruct((8, LANES), jnp.float32),
        ),
        in_specs=[ANY] * (len(lead) + len(rest)) + [VMEM] * 4,
        out_specs=(VMEM, VMEM),
        scratch_shapes=[pltpu.SemaphoreType.DMA((2, count))],
        compiler_params=pltpu.CompilerParams(vmem_limit_bytes=32 << 20),
        cost_estimate=pl.CostEstimate(
            flops=6 * 10**9, bytes_accessed=14 * 10**6, transcendentals=0
        ),
        name="row_panel",
    )(*lead, *rest, qh, ql, low, noise)


def schur_kernel(layout, tiles, features, x_ref, *refs):
    cols = refs[: layout.cols]
    qh_ref, ql_ref, noise_ref, out_ref, y = refs[layout.cols :]
    width = cols[0].shape[1]
    size = qh_ref.shape[0]
    chunks = size // CHUNK
    row, col, feat = (lax.axis_index(name) for name in ("row", "col", "feat"))
    step = pl.program_id(0)
    tile, chunk = step // chunks, lax.rem(step, chunks)

    @pl.when(step == 0)
    def _():
        for m in range(tiles):
            here = pl.ds(m * width, width)
            for k in range(layout.cols):
                for j in range(layout.inner):
                    y[here, pl.ds(layout.offset(k, j), layout.width)] = cols[k][
                        m, :, j * layout.width : (j + 1) * layout.width
                    ]
            points = y[here, :features]
            panel = dot(points, qh_ref[...], NT) + dot(points, ql_ref[...], NT)
            high, low = split(-panel)
            y[here, features : features + size] = high
            y[here, features + size : features + 2 * size] = high
            y[here, features + 2 * size :] = low

    stride = tiles * width // LANES
    for m in range(tiles):

        def store(value):
            for n in range(width // LANES):
                out_ref[pl.ds(m * (width // LANES) + n, CHUNK, stride), :] = value[
                    :, n * LANES : (n + 1) * LANES
                ]

        low_tile = (m < tile) | ((m == tile) & (row >= col))
        first = (col == 0) & low_tile if m == 0 else False

        if m == 0:

            @pl.when(first)
            def _():
                at = pl.multiple_of(feat * width, LANES)
                high = x_ref[0, :, pl.ds(features + at, width)].astype(jnp.float32)
                low = x_ref[0, :, pl.ds(features + size + at, width)].astype(jnp.float32)
                store(high + low)

        @pl.when(low_tile & jnp.logical_not(first))
        def _():
            left = jnp.concatenate([x_ref[0], x_ref[0, :, features : features + size]], axis=1)
            value = dot(left, y[pl.ds(m * width, width), :], NT)
            noise = noise_ref[m : m + 1, pl.ds(pl.multiple_of(feat * width, LANES), width)]
            shape = (CHUNK, width)
            i = chunk * CHUNK + lax.broadcasted_iota(jnp.int32, shape, 0)
            j = feat * width + lax.broadcasted_iota(jnp.int32, shape, 1)
            same = (i == j) & ((m == tile) & (row == col))
            store(value + jnp.where(same, noise, 0.0))

        @pl.when(jnp.logical_not(low_tile))
        def _():
            store(jnp.zeros((CHUNK, width), jnp.float32))


def schur(layout, x, cols, factors, noise):
    qh, ql, _ = factors
    tiles, size = noise.shape
    features = qh.shape[1]
    width = cols[0].shape[1]
    chunks = size // CHUNK
    block = CHUNK * tiles * width // LANES
    steps = tiles * chunks
    return pl.pallas_call(
        functools.partial(schur_kernel, layout, tiles, features),
        grid=(steps,),
        out_shape=jax.ShapeDtypeStruct((steps * block, LANES), jnp.float32),
        in_specs=[
            pl.BlockSpec(
                (1, CHUNK, x.shape[2]), lambda s: (s // chunks, lax.rem(s, chunks), 0)
            )
        ]
        + [VMEM] * (len(cols) + 3),
        out_specs=pl.BlockSpec((block, LANES), lambda s: (s, 0)),
        scratch_shapes=[pltpu.VMEM((tiles * width, features + 3 * size), jnp.bfloat16)],
        compiler_params=pltpu.CompilerParams(vmem_limit_bytes=32 << 20),
        cost_estimate=pl.CostEstimate(
            flops=12 * 10**9, bytes_accessed=20 * 10**6, transcendentals=0
        ),
        name="schur",
    )(x, *cols, qh, ql, noise)


def shift(x, axis, by):
    size = lax.axis_size(axis)
    return lax.ppermute(x, axis, [(i, (i + by) % size) for i in range(size)])


def out_of_row(x, root):
    row_count = lax.axis_size("row")
    row = lax.axis_index("row")
    found = jnp.where(row == root, x, jnp.zeros_like(x))
    for target in range(row_count):
        if target != root:
            found = found + lax.ppermute(x, "row", [(root, target)])
    return found


def from_diagonal(x):
    row_count, col_count = lax.axis_size("row"), lax.axis_size("col")
    held = {0: x}
    away = lax.axis_index("row") ^ lax.axis_index("col")
    found = jnp.where(away == 0, x, jnp.zeros_like(x))
    order = sorted(range(1, row_count), key=lambda n: (bin(n).count("1"), n))
    for target in order:
        source = target & (target - 1)
        pairs = [
            ((c ^ source) * col_count + c, (c ^ target) * col_count + c) for c in range(col_count)
        ]
        held[target] = lax.ppermute(held[source], ("row", "col"), pairs)
        found = found + held[target]
    return found


def shards(points, point_noise):
    row_count, col_count = lax.axis_size("row"), lax.axis_size("col")
    feat_count = lax.axis_size("feat")
    feat = lax.axis_index("feat")
    own, noise = points[:, 0], point_noise[:, 0]
    tiles, size, part = own.shape
    layout = Layout(part)
    features = part * col_count * feat_count
    width = size // feat_count

    steps = sorted(range(1, col_count), key=lambda k: min(k, col_count - k))
    lead, rest = {0: own[0]}, {0: own[1:]}
    for k in steps:
        lead[k] = shift(own[0], "col", k)
    for k in steps:
        rest[k] = shift(own[1:], "col", k)
    lead = jnp.stack([lead[k] for k in range(col_count)])

    def over_feat(x):
        return [x] + [shift(x, "feat", feat_count - j) for j in range(1, feat_count)]

    first_noise = out_of_row(noise[:1], 0)
    first = layout.units(over_feat(out_of_row(lead, 0)))
    lead_parts = over_feat(lead)
    rest_parts = [over_feat(rest[k]) for k in range(col_count)]

    *factors, log_diagonal = factor(layout, first, first_noise, features)

    lead_units = layout.units(lead_parts)
    rest_units = [layout.units(parts) for parts in rest_parts]
    row_rest = [rest_units[k][j] for j in range(layout.inner) for k in range(col_count)]
    x, partial = row_panel(layout, lead_units, row_rest, factors, noise)

    cols = []
    for k in range(col_count):
        whole = [
            jnp.concatenate([lead_units[j][k][None], rest_units[k][j]], axis=0)
            for j in range(layout.inner)
        ]
        half = [lax.dynamic_slice_in_dim(u, feat * width, width, 1) for u in whole]
        cols.append(from_diagonal(jnp.concatenate(half, axis=2)))

    partial = jnp.sum(partial[0])
    row = lax.axis_index("row")
    partials = jnp.zeros((row_count, LANES), jnp.float32)
    for by in range(row_count):
        got = jnp.full((1, LANES), partial) if by == 0 else shift(
            jnp.full((1, LANES), partial), "row", by
        )
        place = lax.rem(row + (row_count - by), row_count)
        partials = lax.dynamic_update_slice(partials, got, (place, 0))
    trace = partials[0, 0]
    for n in range(1, row_count):
        trace = trace + partials[n, 0]
    trace_mean = trace / jnp.float32((tiles * row_count - 1) * size)

    out = schur(layout, x, cols, factors, noise)
    return (
        out.reshape(tiles, 1, size, tiles, 1, width),
        trace_mean,
        log_diagonal[0, 0],
    )


def solution(mesh):
    placed = (P(None, "row", None, ("col", "feat")), P(None, "row", None))
    return jax.shard_map(
        shards,
        mesh=mesh,
        in_specs=placed,
        out_specs=(P(None, "row", None, None, "col", "feat"), P(), P()),
        check_vma=False,
    )
```

```python
import functools

import jax
import jax.numpy as jnp
from jax import lax
from jax.experimental import pallas as pl
from jax.experimental.pallas import tpu as pltpu
from jax.sharding import PartitionSpec as P


HIGHEST = lax.Precision.HIGHEST
NN = (((1,), (0,)), ((), ()))
NT = (((1,), (1,)), ((), ()))
TN = (((0,), (0,)), ((), ()))
GROUP = 8
BLOCK = 128
LANES = 128
FACTOR_PARTS = (0, 1, 2)
VMEM = pl.BlockSpec(memory_space=pltpu.VMEM)
SMEM = pl.BlockSpec(memory_space=pltpu.SMEM)
ANY = pl.BlockSpec(memory_space=pltpu.HBM)


def split(x):
    high = x.astype(jnp.bfloat16)
    return high, (x - high.astype(jnp.float32)).astype(jnp.bfloat16)


def dot(a, b, dims, precision=None):
    return lax.dot_general(a, b, dims, precision=precision, preferred_element_type=jnp.float32)


class Layout:
    def __init__(self, width):
        self.cols, self.feats = lax.axis_size("col"), lax.axis_size("feat")
        self.apart = width % LANES == 0
        self.width = width if self.apart else width * self.feats
        self.inner = self.feats if self.apart else 1

    def offset(self, k, j):
        place = lax.rem(lax.axis_index("col") + (self.cols - k), self.cols) * self.inner
        if self.apart:
            place = place + lax.rem(lax.axis_index("feat") + j, self.feats)
        return pl.multiple_of(place * self.width, LANES)

    def units(self, parts):
        if self.apart:
            return parts
        turned = jnp.roll(jnp.stack(parts), lax.axis_index("feat"), axis=0)
        return [jnp.concatenate(list(turned), axis=-1)]


def factor_block(a_ref, w_ref):
    shape = (GROUP, BLOCK)
    sub = lax.broadcasted_iota(jnp.int32, shape, 0)

    def rows(x, k):
        return jnp.broadcast_to(x[k : k + 1, :], shape)

    def lanes(x, k):
        return jnp.broadcast_to(x[:, k : k + 1], shape)

    for first in range(0, BLOCK, GROUP):
        group = pl.ds(first, GROUP)
        a, w = a_ref[group, :], w_ref[group, :]
        cols = [lanes(a, first + j) for j in range(GROUP)]
        e = {(k, j): rows(cols[j], k) for j in range(GROUP) for k in range(j, GROUP)}
        inv, low = [], {}
        for j in range(GROUP):
            inv.append(lax.rsqrt(e[j, j]))
            for k in range(j + 1, GROUP):
                low[k, j] = e[k, j] * inv[j]
            for m in range(j + 1, GROUP):
                for k in range(m, GROUP):
                    e[k, m] = e[k, m] - low[k, j] * low[m, j]
        y, yw = [], []
        for k in range(GROUP):
            ra, rw = rows(a, k), rows(w, k)
            for j in range(k):
                ra = ra - low[k, j] * y[j]
                rw = rw - low[k, j] * yw[j]
            y.append(ra * inv[k])
            yw.append(rw * inv[k])
        na, nw = y[0], yw[0]
        for k in range(1, GROUP):
            na = jnp.where(sub == k, y[k], na)
            nw = jnp.where(sub == k, yw[k], nw)
        a_ref[group, :] = na
        w_ref[group, :] = nw
        for after in range(first + GROUP, BLOCK, GROUP):
            under = pl.ds(after, GROUP)
            a, w = a_ref[under, :], w_ref[under, :]
            c = []
            for j in range(GROUP):
                x = lanes(a, first + j)
                for m in range(j):
                    x = x - c[m] * low[j, m]
                c.append(x * inv[j])
            for j in range(GROUP):
                a = a - c[j] * y[j]
                w = w - c[j] * yw[j]
            a_ref[under, :] = a
            w_ref[under, :] = w


def factor_kernel(layout, lo, hi, *refs):
    refs = list(refs)
    take = lambda n: [refs.pop(0) for _ in range(n)]
    blocks = None
    begin = lo == 0
    lead = take(layout.inner) if begin or hi is None else []
    noise_ref = take(1)[0] if begin else None
    state = [] if begin else take(2)
    outs = take(4 if hi is None else 2)
    p, a, w, da, dw, sems, state_sems = refs
    size = a.shape[0]
    blocks = size // BLOCK
    last, hi = hi is None, blocks if hi is None else hi
    copies = []
    for j in range(len(lead)):
        for k in range(layout.cols):
            there = p.at[:, pl.ds(layout.offset(k, j), layout.width)]
            n = j * layout.cols + k
            copies.append(pltpu.make_async_copy(lead[j].at[k], there, sems.at[n]))
    stored = [
        pltpu.make_async_copy(ref, there, state_sems.at[n])
        for n, (ref, there) in enumerate(zip(state, (a, w)))
    ]
    for copy in stored + copies:
        copy.start()
    for copy in stored:
        copy.wait()
    down = lax.broadcasted_iota(jnp.int32, (size, size), 0)
    across = lax.broadcasted_iota(jnp.int32, (size, size), 1)
    eye = down == across
    if begin:
        for copy in copies:
            copy.wait()
        points = p[...]
        a[...] = dot(points, points, NT) + jnp.where(eye, noise_ref[...], 0.0)
        w[...] = jnp.where(eye, 1.0, 0.0)

    def step(n, carry):
        at = pl.ds(pl.multiple_of(n * BLOCK, BLOCK), BLOCK)
        da[...] = a[at, at]
        dw[...] = w[at, at]
        factor_block(da, dw)
        a[at, at] = da[...]
        for m in range(lo, hi):
            low, high = m * BLOCK, (m + 1) * BLOCK

            @pl.when(n == m)
            def _():
                inverse = dw[...]
                if m:
                    w[low:high, :low] = dot(inverse, w[low:high, :low], NN, HIGHEST)
                w[low:high, low:high] = inverse
                if high < size:
                    y = dot(inverse, a[low:high, high:], NN, HIGHEST)
                    a[low:high, high:] = y
                    a[high:, high:] = a[high:, high:] - dot(y, y, TN, HIGHEST)
                    w[high:, :high] = w[high:, :high] - dot(y, w[low:high, :high], TN, HIGHEST)

        return carry

    lax.fori_loop(lo, hi, step, 0)
    if not last:
        written = [
            pltpu.make_async_copy(here, ref, state_sems.at[n])
            for n, (ref, here) in enumerate(zip(outs, (a, w)))
        ]
        for copy in written:
            copy.start()
        for copy in written:
            copy.wait()
        return
    qh_ref, ql_ref, l_ref, log_ref = outs
    upper = a[...]
    logs = jnp.where(eye, jnp.log(jnp.where(eye, upper, 1.0)), 0.0)
    log_ref[0, 0] = 2.0 * jnp.sum(logs)
    l_ref[...] = jnp.where(down <= across, upper, 0.0).T
    inverse = jnp.where(down >= across, w[...], 0.0)
    first = inverse.astype(jnp.bfloat16)
    second, third = split(inverse - first.astype(jnp.float32))
    if not begin:
        for copy in copies:
            copy.wait()
    points = p[...]
    q = dot(first, points, NN) + dot(second, points, NN) + dot(third, points, NN)
    qh_ref[...], ql_ref[...] = split(q)


def factor(layout, lead, noise, features):
    size = noise.shape[-1]
    f32, bf16 = jnp.float32, jnp.bfloat16
    square = jax.ShapeDtypeStruct((size, size), f32)
    wide = jax.ShapeDtypeStruct((size, features), bf16)
    state = ()
    for lo, hi in zip(FACTOR_PARTS, FACTOR_PARTS[1:] + (None,)):
        ends = lo == 0 or hi is None
        operands = (*(lead if ends else ()), *((noise,) if lo == 0 else state))
        specs = [ANY] * (len(lead) if ends else 0) + ([VMEM] if lo == 0 else [ANY] * 2)
        state = pl.pallas_call(
            functools.partial(factor_kernel, layout, lo, hi),
            out_shape=(square, square)
            if hi is not None
            else (wide, wide, square, jax.ShapeDtypeStruct((1, 1), f32)),
            in_specs=specs,
            out_specs=(ANY,) * 2 if hi is not None else (VMEM,) * 3 + (SMEM,),
            scratch_shapes=[
                pltpu.VMEM((size, features), bf16),
                pltpu.VMEM((size, size), f32),
                pltpu.VMEM((size, size), f32),
                pltpu.VMEM((BLOCK, BLOCK), f32),
                pltpu.VMEM((BLOCK, BLOCK), f32),
                pltpu.SemaphoreType.DMA((layout.cols * layout.inner,)),
                pltpu.SemaphoreType.DMA((2,)),
            ],
                    compiler_params=pltpu.CompilerParams(vmem_limit_bytes=24 << 20),
            cost_estimate=pl.CostEstimate(flops=10**9, bytes_accessed=4 * 10**6, transcendentals=0),
        )(*operands)
    return state


def feature_copies(layout, parts, there, sems):
    copies = []
    for j in range(layout.inner):
        for k in range(layout.cols):
            n = j * layout.cols + k
            lanes = pl.ds(layout.offset(k, j), layout.width)
            copies.append(pltpu.make_async_copy(parts[n], there.at[:, lanes], sems.at[n]))
    return copies


def panel_kernel(layout, tiles, *refs):
    count = layout.cols * layout.inner
    parts = refs[:count]
    qh_in, ql_in, l_in, noise_ref, a_out, trace_ref = refs[count : count + 6]
    p, qh, ql, first, a, sems, in_sems, out_sems = refs[count + 6 :]
    size = first.shape[0]
    row = lax.axis_index("row")
    wanted = [
        pltpu.make_async_copy(there, here, in_sems.at[n])
        for n, (there, here) in enumerate(((qh_in, qh), (ql_in, ql), (l_in, first)))
    ]

    def copies(t):
        return feature_copies(layout, [part.at[t] for part in parts], p.at[t], sems.at[t])

    def written(t):
        return pltpu.make_async_copy(a.at[t], a_out.at[t], out_sems.at[t])

    def fold(x):
        return functools.reduce(
            jnp.add, [x[:, n : n + LANES] for n in range(0, x.shape[1], LANES)]
        )

    for copy in wanted:
        copy.start()
    for t in range(tiles):
        for copy in copies(t):
            copy.start()
    for copy in wanted:
        copy.wait()

    def step(t, trace):
        for copy in copies(t):
            copy.wait()
        leading = (row == 0) & (t == 0)
        points = p[t]
        panel = dot(points, qh[...], NT) + dot(points, ql[...], NT)
        panel = jnp.where(leading, first[...], panel)
        high, low = split(panel)
        a[t, :, :size] = high
        a[t, :, size:] = low
        written(t).start()
        wide = points.astype(jnp.float32)
        noise = noise_ref[pl.ds(t, 1), :]
        total = fold(jnp.sum(wide * wide, axis=0, keepdims=True)) + fold(noise)
        part = total - fold(jnp.sum(panel * panel, axis=0, keepdims=True))
        return trace + jnp.where(leading, jnp.zeros_like(part), part)

    trace = lax.fori_loop(0, tiles, step, jnp.zeros((1, LANES), jnp.float32))
    trace_ref[...] = jnp.broadcast_to(jnp.sum(trace), trace_ref.shape)
    for t in range(tiles):
        written(t).wait()


def row_panel(layout, parts, factors, noise):
    qh, ql, low = factors
    tiles, size = noise.shape
    features = qh.shape[1]
    bf16 = jnp.bfloat16
    count = layout.cols * layout.inner
    return pl.pallas_call(
        functools.partial(panel_kernel, layout, tiles),
        out_shape=(
            jax.ShapeDtypeStruct((tiles, size, 2 * size), bf16),
            jax.ShapeDtypeStruct((8, LANES), jnp.float32),
        ),
        in_specs=[ANY] * (len(parts) + 3) + [VMEM],
        out_specs=(ANY, VMEM),
        scratch_shapes=[
            pltpu.VMEM((tiles, size, features), bf16),
            pltpu.VMEM((size, features), bf16),
            pltpu.VMEM((size, features), bf16),
            pltpu.VMEM((size, size), jnp.float32),
            pltpu.VMEM((tiles, size, 2 * size), bf16),
            pltpu.SemaphoreType.DMA((tiles, count)),
            pltpu.SemaphoreType.DMA((3,)),
            pltpu.SemaphoreType.DMA((tiles,)),
        ],
        compiler_params=pltpu.CompilerParams(vmem_limit_bytes=18 << 20),
        cost_estimate=pl.CostEstimate(
            flops=10**9, bytes_accessed=14 * 10**6, transcendentals=0
        ),
        name="row_panel",
    )(*parts, qh, ql, low, noise)


def schur_kernel(layout, tiles, features, rows_of_mesh, *refs):
    last_bit = rows_of_mesh // 2
    count = layout.cols * layout.inner
    parts, cols = refs[:count], refs[count : count + 2 * layout.cols]
    at = count + 2 * layout.cols
    a_in, qh_in, ql_in, noise_ref, *traces = refs[at : at + 4 + rows_of_mesh]
    out, trace_ref = refs[at + 4 + rows_of_mesh : at + 6 + rows_of_mesh]
    p, a, y, qh, ql, ring, zero, sems, a_sems, col_sems, q_sems, ring_sems, zero_sems = refs[
        at + 6 + rows_of_mesh :
    ]
    size = noise_ref.shape[1]
    width = y.shape[1]
    groups = width // LANES
    row, col, feat = (lax.axis_index(name) for name in ("row", "col", "feat"))

    def put(value, t, m, sem):
        return [
            pltpu.make_async_copy(
                value.at[:, n * LANES : (n + 1) * LANES],
                out.at[pl.ds(t * size, size), m * groups + n, :],
                sem.at[n],
            )
            for n in range(groups)
        ]

    q_copies = [
        pltpu.make_async_copy(qh_in, qh, q_sems.at[0]),
        pltpu.make_async_copy(ql_in, ql, q_sems.at[1]),
    ]
    far = (row ^ col) >= last_bit

    def col_copies(which):
        return [
            pltpu.make_async_copy(
                cols[2 * k + which].at[:, :, j * layout.width : (j + 1) * layout.width],
                y.at[:, :, pl.ds(layout.offset(k, j), layout.width)],
                col_sems.at[k, j],
            )
            for k in range(layout.cols)
            for j in range(layout.inner)
        ]

    @pl.when(jnp.logical_not(far))
    def _():
        for copy in col_copies(0):
            copy.start()

    @pl.when(far)
    def _():
        for copy in col_copies(1):
            copy.start()

    for copy in q_copies:
        copy.start()

    def row_copies(t):
        return [
            *feature_copies(layout, [part.at[t] for part in parts], p.at[t], sems.at[t]),
            pltpu.make_async_copy(a_in.at[t], a.at[t], a_sems.at[t]),
        ]

    for t in range(tiles):
        for copy in row_copies(t):
            copy.start()
    zero[...] = jnp.zeros_like(zero)
    blank, at = [], 0
    for t in range(tiles):
        for m in range(t + 1, tiles):
            blank += put(zero, t, m, zero_sems.at[at])
            at += 1
    trace = jnp.zeros((1, LANES), jnp.float32)
    for n in range(rows_of_mesh):
        back = lax.rem(row + (rows_of_mesh - n), rows_of_mesh)
        for by in range(rows_of_mesh):
            trace = trace + jnp.where(back == by, traces[by][0:1, :], 0.0)
    first_lane = lax.broadcasted_iota(jnp.int32, (1, LANES), 1) == 0
    count = jnp.float32((tiles * rows_of_mesh - 1) * size)
    trace_ref[0, 0] = jnp.sum(jnp.where(first_lane, trace / count, 0.0))
    for copy in col_copies(0) + q_copies:
        copy.wait()
    for copy in blank:
        copy.start()

    def step(t, carry):
        points = y[t, :, :features]
        panel = dot(points, qh[...], NT) + dot(points, ql[...], NT)
        high, low = split(-panel)
        y[t, :, features : features + size] = high
        y[t, :, features + size : features + 2 * size] = high
        y[t, :, features + 2 * size :] = low
        for copy in row_copies(t):
            copy.wait()
        left = jnp.concatenate([p[t], a[t], a[t, :, :size]], axis=1)
        for m in range(tiles):
            here = ring.at[m]
            low_tile = (t > m) | (row >= col)

            @pl.when(t > m)
            def _():
                for copy in put(here, t - 1, m, ring_sems.at[m]):
                    copy.wait()

            def schur_tile():
                value = dot(left, y[m], NT)
                columns = pl.ds(pl.multiple_of(feat * width, LANES), width)
                i = lax.broadcasted_iota(jnp.int32, (size, width), 0)
                j = feat * width + lax.broadcasted_iota(jnp.int32, (size, width), 1)
                same = (i == j) & ((t == m) & (row == col))
                here[...] = value + jnp.where(same, noise_ref[m : m + 1, columns], 0.0)

            def panel_tile():
                start = pl.multiple_of(feat * width, LANES)
                high = a[t, :, pl.ds(start, width)].astype(jnp.float32)
                low = a[t, :, pl.ds(size + start, width)].astype(jnp.float32)
                here[...] = high + low

            def no_tile():
                here[...] = jnp.zeros_like(here)

            reached = t >= m
            if m == 0:
                pl.when(low_tile & (col == 0))(panel_tile)
                pl.when(low_tile & (col > 0))(schur_tile)
            else:
                pl.when(reached & low_tile)(schur_tile)
            pl.when(reached & jnp.logical_not(low_tile))(no_tile)

            @pl.when(reached)
            def _():
                for copy in put(here, t, m, ring_sems.at[m]):
                    copy.start()

        return carry

    lax.fori_loop(0, tiles, step, 0)
    for m in range(tiles):
        for copy in put(ring.at[m], tiles - 1, m, ring_sems.at[m]):
            copy.wait()
    for copy in blank:
        copy.wait()


def schur(layout, parts, cols, a, factors, noise, traces):
    qh, ql, _ = factors
    tiles, size = noise.shape
    features = qh.shape[1]
    width = cols[0].shape[1]
    bf16 = jnp.bfloat16
    groups = width // LANES
    return pl.pallas_call(
        functools.partial(schur_kernel, layout, tiles, features, len(traces)),
        out_shape=(
            jax.ShapeDtypeStruct((tiles * size, tiles * groups, LANES), jnp.float32),
            jax.ShapeDtypeStruct((1, 1), jnp.float32),
        ),
        in_specs=[ANY] * (len(parts) + len(cols) + 3) + [VMEM] * (1 + len(traces)),
        out_specs=(ANY, SMEM),
        scratch_shapes=[
            pltpu.VMEM((tiles, size, features), bf16),
            pltpu.VMEM((tiles, size, 2 * size), bf16),
            pltpu.VMEM((tiles, width, features + 3 * size), bf16),
            pltpu.VMEM((size, features), bf16),
            pltpu.VMEM((size, features), bf16),
            pltpu.VMEM((tiles, size, width), jnp.float32),
            pltpu.VMEM((size, width), jnp.float32),
            pltpu.SemaphoreType.DMA((tiles, len(parts))),
            pltpu.SemaphoreType.DMA((tiles,)),
            pltpu.SemaphoreType.DMA((layout.cols, layout.inner)),
            pltpu.SemaphoreType.DMA((2,)),
            pltpu.SemaphoreType.DMA((tiles, groups)),
            pltpu.SemaphoreType.DMA((max(1, tiles * (tiles - 1) // 2), groups)),
        ],
        compiler_params=pltpu.CompilerParams(vmem_limit_bytes=28 << 20),
        cost_estimate=pl.CostEstimate(
            flops=10**9, bytes_accessed=20 * 10**6, transcendentals=0
        ),
        name="schur",
    )(*parts, *cols, a, qh, ql, noise, *traces)


def shift(x, axis, by):
    size = lax.axis_size(axis)
    return lax.ppermute(x, axis, [(i, (i + by) % size) for i in range(size)])


def out_of_first_row(x):
    found = jnp.where(lax.axis_index("row") == 0, x, jnp.zeros_like(x))
    for target in range(1, lax.axis_size("row")):
        found = found + lax.ppermute(x, "row", [(0, target)])
    return found


def with_noise(points, noise):
    first = lax.reduce_precision(noise, 8, 7)
    second = lax.reduce_precision(noise - first, 8, 7)
    flat = jnp.concatenate([first, second, noise - first - second]).astype(jnp.bfloat16)
    width = points.shape[1]
    flat = jnp.pad(flat, (0, -flat.size % (16 * width)))
    return jnp.concatenate([points, flat.reshape(-1, width)])


def noise_of(x, size):
    return jnp.sum(x[size:].reshape(-1)[: 3 * size].reshape(3, size).astype(jnp.float32), axis=0)


def around(own, near):
    count = lax.axis_size("col")
    held = {0: own}
    for k in near:
        by = 1 if 2 * k <= count else -1
        held[k] = shift(held[(k - by) % count], "col", by)
    return [held[k] for k in range(count)]


def down_tree(x):
    row_count, col_count = lax.axis_size("row"), lax.axis_size("col")
    away = lax.axis_index("row") ^ lax.axis_index("col")
    bit, got = 1, x
    while bit < row_count:
        if bit > 1:
            x = jnp.where((away >= bit // 2) & (away < bit), got, x)
        pairs = [
            ((c ^ q) * col_count + c, (c ^ q ^ bit) * col_count + c)
            for c in range(col_count)
            for q in range(bit)
        ]
        got = lax.ppermute(x, ("row", "col"), pairs)
        bit = bit * 2
    return x, got


def hops(col_count):
    return sorted(range(1, col_count), key=lambda k: (min(k, col_count - k), k))


def whole(points, point_noise):
    row_count, col_count = lax.axis_size("row"), lax.axis_size("col")
    feat_count = lax.axis_size("feat")
    feat = lax.axis_index("feat")
    own, noise = points[:, 0], point_noise[:, 0]
    tiles, size, part = own.shape
    layout = Layout(part)
    features = part * col_count * feat_count
    width = size // feat_count
    near = hops(col_count)

    def over_feat(x):
        return [x] + [shift(x, "feat", feat_count - j) for j in range(1, feat_count)]

    slices = out_of_first_row(with_noise(own[0], noise[0]))
    first_noise = noise_of(slices, size)[None]
    own_slice = slices[:size]
    stack = jnp.stack([own_slice] + [shift(own_slice, "col", k) for k in range(1, col_count)])
    first = layout.units(over_feat(stack))
    units = [layout.units(over_feat(part)) for part in around(own, near)]

    cols = []
    for k in range(col_count):
        half = [lax.dynamic_slice_in_dim(unit, feat * width, width, 1) for unit in units[k]]
        cols += down_tree(jnp.concatenate(half, axis=2))

    *factors, log_diagonal = factor(layout, first, first_noise, features)
    parts = [units[k][j] for j in range(layout.inner) for k in range(col_count)]
    a, partial = row_panel(layout, parts, factors, noise)
    traces = [shift(partial, "row", by) if by else partial for by in range(row_count)]

    out, trace = schur(layout, parts, cols, a, factors, noise, traces)
    return (
        out.reshape(tiles, 1, size, tiles, 1, width),
        trace.reshape(()),
        log_diagonal.reshape(()),
    )


def solution(mesh):
    placed = (P(None, "row", None, ("col", "feat")), P(None, "row", None))
    return jax.shard_map(
        whole,
        mesh=mesh,
        in_specs=placed,
        out_specs=(P(None, "row", None, None, "col", "feat"), P(), P()),
        check_vma=False,
    )
```

```python
import functools

import jax
import jax.numpy as jnp
from jax import lax
from jax.experimental import pallas as pl
from jax.experimental.pallas import tpu as pltpu
from jax.sharding import PartitionSpec as P


HIGHEST = lax.Precision.HIGHEST
NN = (((1,), (0,)), ((), ()))
NT = (((1,), (1,)), ((), ()))
TN = (((0,), (0,)), ((), ()))
GROUP = 8
BLOCK = 128
LANES = 128
FACTOR_PARTS = (0, 1, 2)
VMEM = pl.BlockSpec(memory_space=pltpu.VMEM)
SMEM = pl.BlockSpec(memory_space=pltpu.SMEM)
ANY = pl.BlockSpec(memory_space=pltpu.HBM)


def split(x):
    high = x.astype(jnp.bfloat16)
    return high, (x - high.astype(jnp.float32)).astype(jnp.bfloat16)


def dot(a, b, dims, precision=None):
    return lax.dot_general(a, b, dims, precision=precision, preferred_element_type=jnp.float32)


class Layout:
    def __init__(self, width):
        self.cols, self.feats = lax.axis_size("col"), lax.axis_size("feat")
        self.apart = width % LANES == 0
        self.width = width if self.apart else width * self.feats
        self.inner = self.feats if self.apart else 1

    def offset(self, k, j):
        place = lax.rem(lax.axis_index("col") + (self.cols - k), self.cols) * self.inner
        if self.apart:
            place = place + lax.rem(lax.axis_index("feat") + j, self.feats)
        return pl.multiple_of(place * self.width, LANES)

    def units(self, parts):
        if self.apart:
            return parts
        turned = jnp.roll(jnp.stack(parts), lax.axis_index("feat"), axis=0)
        return [jnp.concatenate(list(turned), axis=-1)]


def factor_block(a_ref, w_ref):
    shape = (GROUP, BLOCK)
    sub = lax.broadcasted_iota(jnp.int32, shape, 0)

    def rows(x, k):
        return jnp.broadcast_to(x[k : k + 1, :], shape)

    def lanes(x, k):
        return jnp.broadcast_to(x[:, k : k + 1], shape)

    for first in range(0, BLOCK, GROUP):
        group = pl.ds(first, GROUP)
        a, w = a_ref[group, :], w_ref[group, :]
        cols = [lanes(a, first + j) for j in range(GROUP)]
        e = {(k, j): rows(cols[j], k) for j in range(GROUP) for k in range(j, GROUP)}
        inv, low = [], {}
        for j in range(GROUP):
            inv.append(lax.rsqrt(e[j, j]))
            for k in range(j + 1, GROUP):
                low[k, j] = e[k, j] * inv[j]
            for m in range(j + 1, GROUP):
                for k in range(m, GROUP):
                    e[k, m] = e[k, m] - low[k, j] * low[m, j]
        y, yw = [], []
        for k in range(GROUP):
            ra, rw = rows(a, k), rows(w, k)
            for j in range(k):
                ra = ra - low[k, j] * y[j]
                rw = rw - low[k, j] * yw[j]
            y.append(ra * inv[k])
            yw.append(rw * inv[k])
        na, nw = y[0], yw[0]
        for k in range(1, GROUP):
            na = jnp.where(sub == k, y[k], na)
            nw = jnp.where(sub == k, yw[k], nw)
        a_ref[group, :] = na
        w_ref[group, :] = nw
        for after in range(first + GROUP, BLOCK, GROUP):
            under = pl.ds(after, GROUP)
            a, w = a_ref[under, :], w_ref[under, :]
            c = []
            for j in range(GROUP):
                x = lanes(a, first + j)
                for m in range(j):
                    x = x - c[m] * low[j, m]
                c.append(x * inv[j])
            for j in range(GROUP):
                a = a - c[j] * y[j]
                w = w - c[j] * yw[j]
            a_ref[under, :] = a
            w_ref[under, :] = w


def factor_kernel(layout, lo, hi, *refs):
    refs = list(refs)
    take = lambda n: [refs.pop(0) for _ in range(n)]
    blocks = None
    begin = lo == 0
    lead = take(layout.inner) if begin or hi is None else []
    noise_ref = take(1)[0] if begin else None
    state = [] if begin else [kept.at[n] for kept in take(1) for n in range(2)]
    outs = take(4) if hi is None else [kept.at[n] for kept in take(1) for n in range(2)]
    p, a, w, da, dw, sems, state_sems = refs
    size = a.shape[0]
    blocks = size // BLOCK
    last, hi = hi is None, blocks if hi is None else hi
    copies = []
    for j in range(len(lead)):
        for k in range(layout.cols):
            there = p.at[:, pl.ds(layout.offset(k, j), layout.width)]
            n = j * layout.cols + k
            copies.append(pltpu.make_async_copy(lead[j].at[k], there, sems.at[n]))
    stored = [
        pltpu.make_async_copy(ref, there, state_sems.at[n])
        for n, (ref, there) in enumerate(zip(state, (a, w)))
    ]
    for copy in stored + copies:
        copy.start()
    for copy in stored:
        copy.wait()
    down = lax.broadcasted_iota(jnp.int32, (size, size), 0)
    across = lax.broadcasted_iota(jnp.int32, (size, size), 1)
    eye = down == across
    if begin:
        for copy in copies:
            copy.wait()
        points = p[...]
        a[...] = dot(points, points, NT) + jnp.where(eye, noise_ref[...], 0.0)
        w[...] = jnp.where(eye, 1.0, 0.0)

    def step(n, carry):
        at = pl.ds(pl.multiple_of(n * BLOCK, BLOCK), BLOCK)
        da[...] = a[at, at]
        dw[...] = w[at, at]
        factor_block(da, dw)
        a[at, at] = da[...]
        for m in range(lo, hi):
            low, high = m * BLOCK, (m + 1) * BLOCK

            @pl.when(n == m)
            def _():
                inverse = dw[...]
                if m:
                    w[low:high, :low] = dot(inverse, w[low:high, :low], NN, HIGHEST)
                w[low:high, low:high] = inverse
                if high < size:
                    y = dot(inverse, a[low:high, high:], NN, HIGHEST)
                    a[low:high, high:] = y
                    a[high:, high:] = a[high:, high:] - dot(y, y, TN, HIGHEST)
                    w[high:, :high] = w[high:, :high] - dot(y, w[low:high, :high], TN, HIGHEST)

        return carry

    lax.fori_loop(lo, hi, step, 0)
    if not last:
        written = [
            pltpu.make_async_copy(here, ref, state_sems.at[n])
            for n, (ref, here) in enumerate(zip(outs, (a, w)))
        ]
        for copy in written:
            copy.start()
        for copy in written:
            copy.wait()
        return
    qh_ref, ql_ref, l_ref, log_ref = outs
    upper = a[...]
    logs = jnp.where(eye, jnp.log(jnp.where(eye, upper, 1.0)), 0.0)
    log_ref[0, 0] = 2.0 * jnp.sum(logs)
    l_ref[...] = jnp.where(down <= across, upper, 0.0).T
    inverse = jnp.where(down >= across, w[...], 0.0)
    first = inverse.astype(jnp.bfloat16)
    second, third = split(inverse - first.astype(jnp.float32))
    if not begin:
        for copy in copies:
            copy.wait()
    points = p[...]
    q = dot(first, points, NN) + dot(second, points, NN) + dot(third, points, NN)
    qh_ref[...], ql_ref[...] = split(q)


def factor(layout, lead, noise, features):
    size = noise.shape[-1]
    f32, bf16 = jnp.float32, jnp.bfloat16
    square = jax.ShapeDtypeStruct((size, size), f32)
    kept = jax.ShapeDtypeStruct((2, size, size), f32)
    wide = jax.ShapeDtypeStruct((size, features), bf16)
    state = ()
    for lo, hi in zip(FACTOR_PARTS, FACTOR_PARTS[1:] + (None,)):
        ends = lo == 0 or hi is None
        operands = (*(lead if ends else ()), *((noise,) if lo == 0 else state))
        specs = [ANY] * (len(lead) if ends else 0) + [VMEM if lo == 0 else ANY]
        state = pl.pallas_call(
            functools.partial(factor_kernel, layout, lo, hi),
            out_shape=(kept,)
            if hi is not None
            else (wide, wide, square, jax.ShapeDtypeStruct((1, 1), f32)),
            in_specs=specs,
            out_specs=(ANY,) if hi is not None else (VMEM,) * 3 + (SMEM,),
            scratch_shapes=[
                pltpu.VMEM((size, features), bf16),
                pltpu.VMEM((size, size), f32),
                pltpu.VMEM((size, size), f32),
                pltpu.VMEM((BLOCK, BLOCK), f32),
                pltpu.VMEM((BLOCK, BLOCK), f32),
                pltpu.SemaphoreType.DMA((layout.cols * layout.inner,)),
                pltpu.SemaphoreType.DMA((2,)),
            ],
                    compiler_params=pltpu.CompilerParams(vmem_limit_bytes=24 << 20),
            cost_estimate=pl.CostEstimate(flops=10**9, bytes_accessed=4 * 10**6, transcendentals=0),
        )(*operands)
    return state


def feature_copies(layout, parts, there, sems):
    copies = []
    for j in range(layout.inner):
        for k in range(layout.cols):
            n = j * layout.cols + k
            lanes = pl.ds(layout.offset(k, j), layout.width)
            copies.append(pltpu.make_async_copy(parts[n], there.at[:, lanes], sems.at[n]))
    return copies


def panel_kernel(layout, tiles, *refs):
    count = layout.cols * layout.inner
    parts = refs[:count]
    qh_in, ql_in, l_in, noise_ref, a_out, trace_ref = refs[count : count + 6]
    p, qh, ql, first, a, sems, in_sems, out_sems = refs[count + 6 :]
    size = first.shape[0]
    row = lax.axis_index("row")
    wanted = [
        pltpu.make_async_copy(there, here, in_sems.at[n])
        for n, (there, here) in enumerate(((qh_in, qh), (ql_in, ql), (l_in, first)))
    ]

    def copies(t):
        return feature_copies(layout, [part.at[t] for part in parts], p.at[t], sems.at[t])

    def written(t):
        return pltpu.make_async_copy(a.at[t], a_out.at[t], out_sems.at[t])

    def fold(x):
        return functools.reduce(
            jnp.add, [x[:, n : n + LANES] for n in range(0, x.shape[1], LANES)]
        )

    for copy in wanted:
        copy.start()
    for t in range(tiles):
        for copy in copies(t):
            copy.start()
    for copy in wanted:
        copy.wait()

    def step(t, trace):
        for copy in copies(t):
            copy.wait()
        leading = (row == 0) & (t == 0)
        points = p[t]
        panel = dot(points, qh[...], NT) + dot(points, ql[...], NT)
        panel = jnp.where(leading, first[...], panel)
        high, low = split(panel)
        a[t, :, :size] = high
        a[t, :, size:] = low
        written(t).start()
        wide = points.astype(jnp.float32)
        noise = noise_ref[pl.ds(t, 1), :]
        total = fold(jnp.sum(wide * wide, axis=0, keepdims=True)) + fold(noise)
        part = total - fold(jnp.sum(panel * panel, axis=0, keepdims=True))
        return trace + jnp.where(leading, jnp.zeros_like(part), part)

    trace = lax.fori_loop(0, tiles, step, jnp.zeros((1, LANES), jnp.float32))
    trace_ref[...] = jnp.broadcast_to(jnp.sum(trace), trace_ref.shape)
    for t in range(tiles):
        written(t).wait()


def row_panel(layout, parts, factors, noise):
    qh, ql, low = factors
    tiles, size = noise.shape
    features = qh.shape[1]
    bf16 = jnp.bfloat16
    count = layout.cols * layout.inner
    return pl.pallas_call(
        functools.partial(panel_kernel, layout, tiles),
        out_shape=(
            jax.ShapeDtypeStruct((tiles, size, 2 * size), bf16),
            jax.ShapeDtypeStruct((8, LANES), jnp.float32),
        ),
        in_specs=[ANY] * (len(parts) + 3) + [VMEM],
        out_specs=(ANY, VMEM),
        scratch_shapes=[
            pltpu.VMEM((tiles, size, features), bf16),
            pltpu.VMEM((size, features), bf16),
            pltpu.VMEM((size, features), bf16),
            pltpu.VMEM((size, size), jnp.float32),
            pltpu.VMEM((tiles, size, 2 * size), bf16),
            pltpu.SemaphoreType.DMA((tiles, count)),
            pltpu.SemaphoreType.DMA((3,)),
            pltpu.SemaphoreType.DMA((tiles,)),
        ],
        compiler_params=pltpu.CompilerParams(vmem_limit_bytes=18 << 20),
        cost_estimate=pl.CostEstimate(
            flops=10**9, bytes_accessed=14 * 10**6, transcendentals=0
        ),
        name="row_panel",
    )(*parts, qh, ql, low, noise)


def schur_kernel(layout, tiles, features, rows_of_mesh, *refs):
    last_bit = rows_of_mesh // 2
    count = layout.cols * layout.inner
    parts, cols = refs[:count], refs[count : count + 2 * layout.cols]
    at = count + 2 * layout.cols
    a_in, qh_in, ql_in, noise_ref, *traces = refs[at : at + 4 + rows_of_mesh]
    out, trace_ref = refs[at + 4 + rows_of_mesh : at + 6 + rows_of_mesh]
    p, a, y, qh, ql, ring, zero, sems, a_sems, col_sems, q_sems, ring_sems, zero_sems = refs[
        at + 6 + rows_of_mesh :
    ]
    size = noise_ref.shape[1]
    width = y.shape[1]
    groups = width // LANES
    row, col, feat = (lax.axis_index(name) for name in ("row", "col", "feat"))

    def put(value, t, m, sem):
        return [
            pltpu.make_async_copy(
                value.at[:, n * LANES : (n + 1) * LANES],
                out.at[pl.ds(t * size, size), m * groups + n, :],
                sem.at[n],
            )
            for n in range(groups)
        ]

    q_copies = [
        pltpu.make_async_copy(qh_in, qh, q_sems.at[0]),
        pltpu.make_async_copy(ql_in, ql, q_sems.at[1]),
    ]
    far = (row ^ col) >= last_bit

    def col_copies(which):
        return [
            pltpu.make_async_copy(
                cols[2 * k + which].at[:, :, j * layout.width : (j + 1) * layout.width],
                y.at[:, :, pl.ds(layout.offset(k, j), layout.width)],
                col_sems.at[k, j],
            )
            for k in range(layout.cols)
            for j in range(layout.inner)
        ]

    @pl.when(jnp.logical_not(far))
    def _():
        for copy in col_copies(0):
            copy.start()

    @pl.when(far)
    def _():
        for copy in col_copies(1):
            copy.start()

    for copy in q_copies:
        copy.start()

    def row_copies(t):
        return [
            *feature_copies(layout, [part.at[t] for part in parts], p.at[t], sems.at[t]),
            pltpu.make_async_copy(a_in.at[t], a.at[t], a_sems.at[t]),
        ]

    for t in range(tiles):
        for copy in row_copies(t):
            copy.start()
    zero[...] = jnp.zeros_like(zero)
    blank, at = [], 0
    for t in range(tiles):
        for m in range(t + 1, tiles):
            blank += put(zero, t, m, zero_sems.at[at])
            at += 1
    trace = jnp.zeros((1, LANES), jnp.float32)
    for n in range(rows_of_mesh):
        back = lax.rem(row + (rows_of_mesh - n), rows_of_mesh)
        for by in range(rows_of_mesh):
            trace = trace + jnp.where(back == by, traces[by][0:1, :], 0.0)
    first_lane = lax.broadcasted_iota(jnp.int32, (1, LANES), 1) == 0
    count = jnp.float32((tiles * rows_of_mesh - 1) * size)
    trace_ref[0, 0] = jnp.sum(jnp.where(first_lane, trace / count, 0.0))
    for copy in col_copies(0) + q_copies:
        copy.wait()
    for copy in blank:
        copy.start()

    def step(t, carry):
        points = y[t, :, :features]
        panel = dot(points, qh[...], NT) + dot(points, ql[...], NT)
        high, low = split(-panel)
        y[t, :, features : features + size] = high
        y[t, :, features + size : features + 2 * size] = high
        y[t, :, features + 2 * size :] = low
        for copy in row_copies(t):
            copy.wait()
        left = jnp.concatenate([p[t], a[t], a[t, :, :size]], axis=1)
        for m in range(tiles):
            here = ring.at[m]
            low_tile = (t > m) | (row >= col)

            @pl.when(t > m)
            def _():
                for copy in put(here, t - 1, m, ring_sems.at[m]):
                    copy.wait()

            def schur_tile():
                value = dot(left, y[m], NT)
                columns = pl.ds(pl.multiple_of(feat * width, LANES), width)
                i = lax.broadcasted_iota(jnp.int32, (size, width), 0)
                j = feat * width + lax.broadcasted_iota(jnp.int32, (size, width), 1)
                same = (i == j) & ((t == m) & (row == col))
                here[...] = value + jnp.where(same, noise_ref[m : m + 1, columns], 0.0)

            def panel_tile():
                start = pl.multiple_of(feat * width, LANES)
                high = a[t, :, pl.ds(start, width)].astype(jnp.float32)
                low = a[t, :, pl.ds(size + start, width)].astype(jnp.float32)
                here[...] = high + low

            def no_tile():
                here[...] = jnp.zeros_like(here)

            reached = t >= m
            if m == 0:
                pl.when(low_tile & (col == 0))(panel_tile)
                pl.when(low_tile & (col > 0))(schur_tile)
            else:
                pl.when(reached & low_tile)(schur_tile)
            pl.when(reached & jnp.logical_not(low_tile))(no_tile)

            @pl.when(reached)
            def _():
                for copy in put(here, t, m, ring_sems.at[m]):
                    copy.start()

        return carry

    lax.fori_loop(0, tiles, step, 0)
    for m in range(tiles):
        for copy in put(ring.at[m], tiles - 1, m, ring_sems.at[m]):
            copy.wait()
    for copy in blank:
        copy.wait()


def schur(layout, parts, cols, a, factors, noise, traces):
    qh, ql, _ = factors
    tiles, size = noise.shape
    features = qh.shape[1]
    width = cols[0].shape[1]
    bf16 = jnp.bfloat16
    groups = width // LANES
    return pl.pallas_call(
        functools.partial(schur_kernel, layout, tiles, features, len(traces)),
        out_shape=(
            jax.ShapeDtypeStruct((tiles * size, tiles * groups, LANES), jnp.float32),
            jax.ShapeDtypeStruct((1, 1), jnp.float32),
        ),
        in_specs=[ANY] * (len(parts) + len(cols) + 3) + [VMEM] * (1 + len(traces)),
        out_specs=(ANY, SMEM),
        scratch_shapes=[
            pltpu.VMEM((tiles, size, features), bf16),
            pltpu.VMEM((tiles, size, 2 * size), bf16),
            pltpu.VMEM((tiles, width, features + 3 * size), bf16),
            pltpu.VMEM((size, features), bf16),
            pltpu.VMEM((size, features), bf16),
            pltpu.VMEM((tiles, size, width), jnp.float32),
            pltpu.VMEM((size, width), jnp.float32),
            pltpu.SemaphoreType.DMA((tiles, len(parts))),
            pltpu.SemaphoreType.DMA((tiles,)),
            pltpu.SemaphoreType.DMA((layout.cols, layout.inner)),
            pltpu.SemaphoreType.DMA((2,)),
            pltpu.SemaphoreType.DMA((tiles, groups)),
            pltpu.SemaphoreType.DMA((max(1, tiles * (tiles - 1) // 2), groups)),
        ],
        compiler_params=pltpu.CompilerParams(vmem_limit_bytes=28 << 20),
        cost_estimate=pl.CostEstimate(
            flops=10**9, bytes_accessed=20 * 10**6, transcendentals=0
        ),
        name="schur",
    )(*parts, *cols, a, qh, ql, noise, *traces)


def shift(x, axis, by):
    size = lax.axis_size(axis)
    return lax.ppermute(x, axis, [(i, (i + by) % size) for i in range(size)])


def out_of_first_row(x):
    found = jnp.where(lax.axis_index("row") == 0, x, jnp.zeros_like(x))
    for target in range(1, lax.axis_size("row")):
        found = found + lax.ppermute(x, "row", [(0, target)])
    return found


def with_noise(points, noise):
    first = lax.reduce_precision(noise, 8, 7)
    second = lax.reduce_precision(noise - first, 8, 7)
    flat = jnp.concatenate([first, second, noise - first - second]).astype(jnp.bfloat16)
    width = points.shape[1]
    flat = jnp.pad(flat, (0, -flat.size % (16 * width)))
    return jnp.concatenate([points, flat.reshape(-1, width)])


def noise_of(x, size):
    return jnp.sum(x[size:].reshape(-1)[: 3 * size].reshape(3, size).astype(jnp.float32), axis=0)


def around(own, near):
    count = lax.axis_size("col")
    held = {0: own}
    for k in near:
        by = 1 if 2 * k <= count else -1
        held[k] = shift(held[(k - by) % count], "col", by)
    return [held[k] for k in range(count)]


def down_tree(x):
    row_count, col_count = lax.axis_size("row"), lax.axis_size("col")
    away = lax.axis_index("row") ^ lax.axis_index("col")
    bit, got = 1, x
    while bit < row_count:
        if bit > 1:
            x = jnp.where((away >= bit // 2) & (away < bit), got, x)
        pairs = [
            ((c ^ q) * col_count + c, (c ^ q ^ bit) * col_count + c)
            for c in range(col_count)
            for q in range(bit)
        ]
        got = lax.ppermute(x, ("row", "col"), pairs)
        bit = bit * 2
    return x, got


def hops(col_count):
    return sorted(range(1, col_count), key=lambda k: (min(k, col_count - k), k))


def whole(points, point_noise):
    row_count, col_count = lax.axis_size("row"), lax.axis_size("col")
    feat_count = lax.axis_size("feat")
    feat = lax.axis_index("feat")
    own, noise = points[:, 0], point_noise[:, 0]
    tiles, size, part = own.shape
    layout = Layout(part)
    features = part * col_count * feat_count
    width = size // feat_count
    near = hops(col_count)

    def over_feat(x):
        return [x] + [shift(x, "feat", feat_count - j) for j in range(1, feat_count)]

    slices = out_of_first_row(with_noise(own[0], noise[0]))
    first_noise = noise_of(slices, size)[None]
    own_slice = slices[:size]
    stack = jnp.stack([own_slice] + [shift(own_slice, "col", k) for k in range(1, col_count)])
    first = layout.units(over_feat(stack))
    units = [layout.units(over_feat(part)) for part in around(own, near)]

    cols = []
    for k in range(col_count):
        half = [lax.dynamic_slice_in_dim(unit, feat * width, width, 1) for unit in units[k]]
        cols += down_tree(jnp.concatenate(half, axis=2))

    *factors, log_diagonal = factor(layout, first, first_noise, features)
    parts = [units[k][j] for j in range(layout.inner) for k in range(col_count)]
    a, partial = row_panel(layout, parts, factors, noise)
    traces = [shift(partial, "row", by) if by else partial for by in range(row_count)]

    out, trace = schur(layout, parts, cols, a, factors, noise, traces)
    return (
        out.reshape(tiles, 1, size, tiles, 1, width),
        trace.reshape(()),
        log_diagonal.reshape(()),
    )


def solution(mesh):
    placed = (P(None, "row", None, ("col", "feat")), P(None, "row", None))
    return jax.shard_map(
        whole,
        mesh=mesh,
        in_specs=placed,
        out_specs=(P(None, "row", None, None, "col", "feat"), P(), P()),
        check_vma=False,
    )
```
